256 devices in a mesh: dp: 16 (over z_lo, x), mp: 16 (over z_hi, y, core).
Axes of the slice: x: 4, y: 4, z: 8 (z_hi: 2, z_lo: 4; z = z_hi * 4 + z_lo), core: 2. Of those that a mesh axis runs over, the one named last changes fastest.
Arguments:
- teacher_states: bfloat16 [1024, 128, 4096], P('dp', None, 'mp'), may hold values from -6 to 6
- teacher_gain: float32 [4096], P('mp'), may hold values from 0.25 to 1.75
- teacher_proj: bfloat16 [4096, 1024], P('mp'), may hold values from -0.09375 to 0.09375
- teacher_mask: int32 [1024, 128], P('dp'), may hold values 0 or 1
- student_states: bfloat16 [8192, 64, 768], P(('dp', 'mp')), may hold values from -6 to 6
- student_gain: float32 [768], replicated, may hold values from 0.25 to 1.75
- student_proj: bfloat16 [768, 1024], replicated, may hold values from -0.21875 to 0.21875
- student_mask: int32 [8192, 64], P(('dp', 'mp')), may hold values 0 or 1
- positive: int32 [8192], P(('dp', 'mp')), may hold values from 0 to 1023
Outputs:
- grad_embed: float32 [8192, 1024], P(('dp', 'mp'))
- grad_states: bfloat16 [8192, 64, 768], P(('dp', 'mp'))
The draws below stay inside these ranges and needn't reach their ends.
All inputs are finite; a program needn't handle non-finite values. No bound on the sum of `teacher_mask` or of `student_mask` on one device may be relied on, other than what follows from the above.
Results may differ from the reference program's by a relative error of at most 0.0085.
Values may be sent and summed in bfloat16 or wider, within the bound.
A program may use at most 128 MiB of HBM per device.

```python
import jax
import jax.numpy as jnp
from jax import lax

D = 4096
E = 1024
DS = 768
LEN = 128
QLEN = 64
PASSAGES = 1024
QUERIES = 8192


def place_ends(result, rng, least, high):
    longest = result.shape.index(max(result.shape))
    spots = []
    for shift in (0, 1):
        where = [jax.random.randint(jax.random.fold_in(rng, axis), (), 0, length) for axis, length in enumerate(result.shape)]
        where[longest] = (where[longest] + shift) % result.shape[longest]
        spots.append(tuple(where))
    return result.at[spots[0]].set(least).at[spots[1]].set(high)


def block_scale(own_key, shape, cuts, least, top_value):
    def one(dim, shards_of):
        heights = jax.random.uniform(jax.random.fold_in(jax.random.fold_in(own_key, 6), dim), (shards_of,), jnp.float32, least / len(cuts), top_value / len(cuts))
        return jnp.repeat(jnp.exp(heights), shape[dim] // shards_of).reshape((-1,) + (1,) * (len(shape) - dim - 1))

    level = one(*cuts[0])
    for cut in cuts[1:]:
        level = level * one(*cut)
    return level


def normal_values(rng, shape, spread, reach, cuts=(), kind=jnp.bfloat16):
    drawn = spread * jax.random.normal(rng, shape, jnp.float32)
    if cuts:
        drawn = drawn * block_scale(rng, shape, cuts, -0.22, 0.18)
    return jnp.clip(drawn, -reach, reach).astype(kind)


def setup_inputs(seed: int = 0) -> dict:
    streams_of = jax.random.split(jax.random.key(seed), 10)
    teacher_states = normal_values(streams_of[0], (PASSAGES, LEN, D), 1.0, 6.0, ((0, 16), (2, 16)))
    teacher_gain = jnp.clip(1.0 + 0.15 * jax.random.normal(streams_of[1], (D,), jnp.float32), 0.25, 1.75)
    teacher_proj = normal_values(streams_of[2], (D, E), D ** -0.5, 0.09375, ((0, 16),))
    teacher_mask = place_ends((jax.random.randint(streams_of[3], (PASSAGES, LEN), 0, 4) < 3).astype(jnp.int32), jax.random.fold_in(streams_of[3], 1), 0, 1)
    student_states = normal_values(streams_of[4], (QUERIES, QLEN, DS), 1.0, 6.0, ((0, 256),))
    student_gain = jnp.clip(1.0 + 0.15 * jax.random.normal(streams_of[5], (DS,), jnp.float32), 0.25, 1.75)
    student_proj = normal_values(streams_of[6], (DS, E), DS ** -0.5, 0.21875)
    student_mask = place_ends((jax.random.randint(streams_of[7], (QUERIES, QLEN), 0, 4) < 3).astype(jnp.int32), jax.random.fold_in(streams_of[7], 1), 0, 1)
    positive = place_ends(jax.random.randint(streams_of[8], (QUERIES,), 0, PASSAGES), jax.random.fold_in(streams_of[8], 1), 0, PASSAGES - 1).astype(jnp.int32)
    return dict(teacher_states=teacher_states, teacher_gain=teacher_gain, teacher_proj=teacher_proj, teacher_mask=teacher_mask, student_states=student_states, student_gain=student_gain, student_proj=student_proj, student_mask=student_mask, positive=positive)


def pool_block(pair):
    states, live_mask = pair
    values = states.astype(jnp.float32)
    scale = lax.rsqrt(lax.optimization_barrier(jnp.mean(values * values, axis=-1)) + 1e-06)
    live = live_mask.astype(jnp.float32)
    weight = live * scale
    return lax.optimization_barrier(jnp.sum(values * weight[:, :, None], axis=1))

def unit_rows(values):
    return values * lax.rsqrt(lax.optimization_barrier(jnp.mean(values * values, axis=-1, keepdims=True)) + 1e-06) / jnp.sqrt(jnp.float32(values.shape[-1]))

def student_forward(states, gain, proj, live_mask):
    values = states.astype(jnp.float32)
    scale = lax.rsqrt(lax.optimization_barrier(jnp.mean(values * values, axis=-1, keepdims=True)) + 1e-06)
    normed = (values * scale * gain).astype(jnp.bfloat16)
    flat = normed.reshape(-1, normed.shape[-1])
    act = jax.nn.gelu(jnp.dot(flat, proj, preferred_element_type=jnp.float32), approximate=True)
    act = act.reshape(states.shape[0], states.shape[1], -1)
    live = live_mask.astype(jnp.float32)
    pooled = lax.optimization_barrier(jnp.sum(act * live[:, :, None], axis=1))
    return unit_rows(pooled)

def reference(teacher_states, teacher_gain, teacher_proj, teacher_mask, student_states, student_gain, student_proj, student_mask, positive):
    blocks = teacher_states.reshape(-1, 16, LEN, D)
    masks = teacher_mask.reshape(-1, 16, LEN)
    pooled = lax.map(pool_block, (blocks, masks)).reshape(PASSAGES, D)
    tpooled = (pooled * teacher_gain).astype(jnp.bfloat16)
    traw = jnp.dot(tpooled, teacher_proj, preferred_element_type=jnp.float32)
    temb = unit_rows(traw).astype(jnp.bfloat16)
    semb, back = jax.vjp(lambda st: student_forward(st, student_gain, student_proj, student_mask), student_states)
    sround = semb.astype(jnp.bfloat16)
    tpos = temb[positive]
    tlogit = 10.0 * jnp.dot(tpos, temb.T, preferred_element_type=jnp.float32)
    slogit = 20.0 * jnp.dot(sround, temb.T, preferred_element_type=jnp.float32)
    texp = jnp.exp(tlogit)
    sexp = jnp.exp(slogit)
    diff = (sexp / lax.optimization_barrier(jnp.sum(sexp, axis=1, keepdims=True)) - texp / lax.optimization_barrier(jnp.sum(texp, axis=1, keepdims=True))).astype(jnp.bfloat16)
    grad_embed = 20.0 * jnp.dot(diff, temb, preferred_element_type=jnp.float32)
    grad_states = back(grad_embed)[0]
    return (grad_embed, grad_states.astype(jnp.bfloat16))
```

```python
import functools

import jax
import jax.numpy as jnp
from jax import lax
from jax.experimental import pallas as pl
from jax.experimental.pallas import tpu as pltpu
from jax.sharding import PartitionSpec as P

D = 4096
F32 = jnp.float32
BF16 = jnp.bfloat16
MESH = pl.DeviceIdType.MESH
NT = (((1,), (1,)), ((), ()))
PARTS = ((0, 384), (384, 384), (768, 256))
GELU_C = 0.7978845608028654
GELU_K = 0.044715


def place():
    d, m = lax.axis_index("dp"), lax.axis_index("mp")
    return lax.div(d, 4), lax.rem(d, 4), lax.div(m, 8), lax.rem(lax.div(m, 2), 4), lax.rem(m, 2)


def student_chunk(i, sx, sproj, sgain, live, gp, praw, sl_out, normed):
    rows = pl.ds(i * 512, 512)
    x = sx[rows, :].astype(F32)
    scale = lax.rsqrt(jnp.sum(x * x, axis=1, keepdims=True) / 768.0 + 1e-06)
    sl = scale * live[:, i : i + 1]
    sl_out[rows, :] = jnp.broadcast_to(sl, (512, 128))
    normed[...] = (x * sl * sgain[...]).astype(BF16)

    def block(n, carry):
        cols = pl.ds(pl.multiple_of(n * 256, 256), 256)
        pre = jnp.dot(normed[...], sproj[:, cols], preferred_element_type=F32)
        sq = pre * pre
        half = 0.5 + 0.5 * jnp.tanh(pre * (GELU_C + (GELU_C * GELU_K) * sq))
        act = pre * half
        gp[rows, cols] = (
            half + act * (1.0 - half) * (2.0 * GELU_C + (6.0 * GELU_C * GELU_K) * sq)
        ).astype(BF16)
        praw[i * 8 : i * 8 + 8, cols] = jnp.sum(act.reshape(8, 64, 256), axis=1)
        return carry

    lax.fori_loop(0, 4, block, 0)


def gather_kernel(
    tx_hbm, tproj_hbm, tgain, tlive, sx_hbm, sproj_hbm, sgain, slive, pos,
    ge, gp, praw, sl_out,
    tx, tproj, sx, sproj, normed,
    sq_own, sq_out, sq_in, sqz_out, sqz_in,
    pe_own, pe_out, pe_in, pez_out, pez_in, T,
    ld_sem, sq_s, sq_r, pe_s, pe_r, z_s, z_r, a1_s, a1_r, a2_s, a2_r, c_s, c_r,
):
    zlo, x, zhi, y, core = place()
    z = zhi * 4 + zlo
    two = 2 - 4 * core

    def dev(zz, xx, yy, cc):
        zz, xx, yy = lax.rem(zz + 8, 8), lax.rem(xx + 4, 4), lax.rem(yy + 4, 4)
        return {"dp": lax.rem(zz, 4) * 4 + xx, "mp": lax.div(zz, 4) * 8 + yy * 2 + cc}

    loads = []
    for k in range(4):
        loads.append(pltpu.make_async_copy(tx_hbm.at[pl.ds(16 * k, 16)], tx.at[pl.ds(16 * k, 16)], ld_sem.at[k]))
    loads.append(pltpu.make_async_copy(sx_hbm, sx, ld_sem.at[4]))
    loads.append(pltpu.make_async_copy(sproj_hbm, sproj, ld_sem.at[5]))
    loads.append(pltpu.make_async_copy(tproj_hbm, tproj, ld_sem.at[6]))
    for c in loads:
        c.start()

    peers = []
    for dz in (0, 1, -1, 2, -2):
        for dy in range(4):
            if (dz, dy) != (0, 0):
                peers.append(dev(z + dz, x, y + dy, core))
        for dx in range(1, 4):
            peers.append(dev(z + dz, x + dx, y, core))
    for dx in range(1, 4):
        for dy in range(1, 4):
            peers.append(dev(z, x + dx, y + dy, core))
    for dy in range(4):
        peers.append(dev(z, x, y + dy, 1 - core))
    peers.append(dev(z + 4, x, y, core))
    barrier = pltpu.get_barrier_semaphore()
    for p in peers:
        pl.semaphore_signal(barrier, inc=1, device_id=p, device_id_type=MESH)

    def remote(src, dst, ss, rs, to):
        return pltpu.make_async_remote_copy(
            src_ref=src, dst_ref=dst, send_sem=ss, recv_sem=rs, device_id=to, device_id_type=MESH
        )

    me = y * 2 + core
    others = [lax.rem(me + k, 8) for k in range(1, 8)]
    sends = []

    def peer8(s):
        return dev(z, x, lax.div(s, 2), lax.rem(s, 2))

    row = lax.broadcasted_iota(jnp.int32, (16, 256), 0)
    for h in range(2):
        total = jnp.zeros((16, 256), F32)
        for q in range(16):
            if q % 8 == 0:
                loads[2 * h + q // 8].wait()
            p = 32 * h + 2 * q
            v = tx[p : p + 2].reshape(256, 256)
            pick = jnp.where(row == q, 1.0, 0.0).astype(BF16)
            total = total + lax.dot_general(pick, v * v, NT, preferred_element_type=F32)
        sq_own[h] = total
        sq_out[h] = total.astype(BF16)
        if h == 0:
            pl.semaphore_wait(barrier, len(peers))
        for s in others:
            c = remote(sq_out.at[h], sq_in.at[h, me], sq_s.at[h, s], sq_r.at[h, me], peer8(s))
            c.start()
            sends.append(c)

    loads[4].wait()
    loads[5].wait()
    student = functools.partial(
        student_chunk, sx=sx, sproj=sproj, sgain=sgain, live=slive, gp=gp, praw=praw, sl_out=sl_out, normed=normed
    )
    student(0)

    partner = dev(z + 4, x, y, core)
    for h in range(2):
        for s in others:
            remote(sq_in.at[h, s], sq_in.at[h, s], sq_s.at[h, s], sq_r.at[h, s], partner).wait_recv()
        total = sq_own[h]
        for s in others:
            total = total + sq_in[h, s].astype(F32)
        sq_own[h] = total
        sqz_out[h] = total.astype(BF16)
    zc = remote(sqz_out, sqz_in, z_s.at[0], z_r.at[0], partner)
    zc.start()
    sends.append(zc)
    student(1)
    zc.wait_recv()

    loads[6].wait()
    row = lax.broadcasted_iota(jnp.int32, (16, 256), 0)
    lane = lax.broadcasted_iota(jnp.int32, (16, 256), 1)
    pooled = []
    for h in range(2):
        squares = sq_own[h] + sqz_in[h].astype(F32)
        weight = tlive[16 * h : 16 * h + 16, :] * lax.rsqrt(squares / D + 1e-06)
        high = weight.astype(BF16).astype(F32)
        low = weight - high
        for g in range(4):
            total = jnp.zeros((16, 256), F32)
            for k in range(4):
                q = 4 * g + k
                both = jnp.where(row < 8, high[q : q + 1, :], low[q : q + 1, :])
                mine = lax.rem(row, 8) == 2 * k + lax.div(lane, 128)
                lhs = jnp.where(mine, both, 0.0).astype(BF16)
                p = 32 * h + 2 * q
                v = tx[p : p + 2].reshape(256, 256)
                total = total + jnp.dot(lhs, v, preferred_element_type=F32)
            pooled.append(total[:8] + total[8:])
    tpooled = (jnp.concatenate(pooled, axis=0) * tgain[...]).astype(BF16)
    partial = jnp.dot(tpooled, tproj[...], preferred_element_type=F32).reshape(8, 8, 1024)
    pe_own[...] = partial
    pe_out[...] = partial.astype(BF16)
    for s in others:
        c = remote(pe_out.at[s], pe_in.at[me], pe_s.at[s], pe_r.at[me], peer8(s))
        c.start()
        sends.append(c)
    student(2)
    for s in others:
        remote(pe_in.at[s], pe_in.at[s], pe_s.at[s], pe_r.at[s], partner).wait_recv()
    total = pe_own[me]
    for s in others:
        total = total + pe_in[s].astype(F32)
    pez_out[...] = total.astype(BF16)
    zc = remote(pez_out, pez_in, z_s.at[1], z_r.at[1], partner)
    zc.start()
    sends.append(zc)
    student(3)
    zc.wait_recv()
    traw = total + pez_in[...].astype(F32)
    scale = lax.rsqrt(jnp.mean(traw * traw, axis=-1, keepdims=True) + 1e-06)
    T[core, zlo, x, y] = (traw * scale / 32.0).astype(BF16)

    zoffs = (0, 1, -1, two)
    ahead = lambda v, k: lax.rem(v + k, 4)

    def plane(part, az, ax, ay):
        lo, n = PARTS[part]
        return T.at[core, az, ax, ay, :, pl.ds(lo, n)]

    slots = (zlo * 4 + y, zlo * 4 + x, x * 4 + y)
    for part in range(3):
        mine = plane(part, zlo, x, y)
        targets = []
        if part == 0:
            targets = [dev(z + zoffs[a], x, y + b, core) for a in range(4) for b in range(4) if a or b]
        elif part == 1:
            targets = [dev(z + zoffs[a], x + b, y, core) for a in range(4) for b in range(4) if a or b]
        else:
            targets = [dev(z, x + a, y + b, core) for a in range(4) for b in range(4) if a or b]
        for k, to in enumerate(targets):
            c = remote(mine, mine, a1_s.at[part, k], a1_r.at[part, slots[part]], to)
            c.start()
            sends.append(c)

    def line(part, cc, v):
        lo, n = PARTS[part]
        cols = pl.ds(lo, n)
        if part == 0:
            return T.at[cc, :, v, :, :, cols]
        if part == 1:
            return T.at[cc, :, :, v, :, cols]
        return T.at[cc, v, :, :, :, cols]

    own_line = (x, y, zlo)
    other = dev(z, x, y, 1 - core)
    for part in range(3):
        mine = plane(part, zlo, x, y)
        for k in range(1, 16):
            s = lax.rem(slots[part] + k, 16)
            remote(mine, mine, a1_s.at[part, k - 1], a1_r.at[part, s], other).wait_recv()
        v = own_line[part]
        src = line(part, core, v)
        if part == 0:
            targets = [dev(z, x + k, y, core) for k in (1, 3, 2)]
        elif part == 1:
            targets = [dev(z, x, y + k, core) for k in (1, 3, 2)]
        else:
            targets = [dev(z + zoffs[k], x, y, core) for k in (1, 2, 3)]
        for k, to in enumerate(targets):
            c = remote(src, src, a2_s.at[part, k], a2_r.at[part, v], to)
            c.start()
            sends.append(c)
        c = remote(src, src, c_s.at[part, v], c_r.at[part, v], other)
        c.start()
        sends.append(c)
    for k in (1, 3, 2):
        for part in range(3):
            v = ahead(own_line[part], k)
            src = line(part, core, v)
            remote(src, src, a2_s.at[part, 0], a2_r.at[part, v], other).wait_recv()
            c = remote(src, src, c_s.at[part, v], c_r.at[part, v], other)
            c.start()
            sends.append(c)
    for part in range(3):
        for v in range(4):
            dst = line(part, 1 - core, v)
            remote(dst, dst, c_s.at[part, v], c_r.at[part, v], other).wait_recv()

    praws = praw[...]
    semb = praws * lax.rsqrt(jnp.mean(praws * praws, axis=-1, keepdims=True) + 1e-06) / 32.0
    temb = T[...].reshape(1024, 1024)
    lanes = lax.broadcasted_iota(jnp.int32, (32, 1024), 1)
    picker = jnp.where(pos[...] == lanes, 1.0, 0.0).astype(BF16)
    tpos = jnp.dot(picker, temb, preferred_element_type=F32).astype(BF16)
    both = jnp.concatenate([tpos, semb.astype(BF16)], axis=0)
    logits = lax.dot_general(both, temb, NT, preferred_element_type=F32)
    texp = jnp.exp(10.0 * logits[:32])
    sexp = jnp.exp(20.0 * logits[32:])
    diff = sexp / jnp.sum(sexp, axis=1, keepdims=True) - texp / jnp.sum(texp, axis=1, keepdims=True)
    ge[...] = 20.0 * jnp.dot(diff.astype(BF16), temb, preferred_element_type=F32)

    for c in sends:
        c.wait_send()


def back_kernel(ge, praw, gp, sl_in, sproj, sgain, sx, ge_hbm, out_hbm, out, st_sem):
    stores = [pltpu.make_async_copy(ge, ge_hbm, st_sem.at[8])]
    stores[0].start()
    p, g = praw[...], ge[...]
    r = lax.rsqrt(jnp.mean(p * p, axis=-1, keepdims=True) + 1e-06)
    ds = (g * r - p * (r * r * r) * jnp.mean(p * g, axis=-1, keepdims=True)) / 32.0
    gain = sgain[...]
    for i in range(8):
        rows = pl.ds(256 * i, 256)
        slope = gp[rows, :].astype(F32).reshape(4, 64, 1024)
        dpre = (slope * ds[4 * i : 4 * i + 4][:, None, :]).reshape(256, 1024).astype(BF16)
        dn = lax.dot_general(dpre, sproj[...], NT, preferred_element_type=F32)
        dy = dn.astype(BF16).astype(F32) * gain
        x = sx[rows, :].astype(F32)
        sl = sl_in[rows, :1]
        m = jnp.sum(x * dy, axis=1, keepdims=True) * (sl * sl / 768.0)
        out[rows, :] = (sl * (dy - x * m)).astype(BF16)
        stores.append(pltpu.make_async_copy(out.at[rows], out_hbm.at[rows], st_sem.at[i]))
        stores[-1].start()
    for c in stores:
        c.wait()


def shards(
    teacher_states, teacher_gain, teacher_proj, teacher_mask,
    student_states, student_gain, student_proj, student_mask, positive,
):
    vmem = pl.BlockSpec(memory_space=pltpu.VMEM)
    hbm = pl.BlockSpec(memory_space=pltpu.HBM)
    dma = pltpu.SemaphoreType.DMA
    in_hbm = lambda a: pltpu.with_memory_space_constraint(a, pltpu.HBM)
    sx = student_states.reshape(2048, 768)
    sgain = student_gain.reshape(1, 768)
    slive = student_mask.astype(F32).reshape(4, 512).T
    tlive = teacher_mask.astype(F32).reshape(32, 256)
    p = positive
    pos = ((p // 8) % 2) * 512 + (p // 256) * 128 + ((p // 64) % 4) * 32 + ((p // 16) % 4) * 8 + p % 8
    ge, gp, praw, sl = pl.pallas_call(
        gather_kernel,
        name="gather",
        out_shape=(
            jax.ShapeDtypeStruct((32, 1024), F32),
            jax.ShapeDtypeStruct((2048, 1024), BF16),
            jax.ShapeDtypeStruct((32, 1024), F32),
            jax.ShapeDtypeStruct((2048, 128), F32),
        ),
        in_specs=[hbm, hbm, vmem, vmem, hbm, hbm, vmem, vmem, vmem],
        out_specs=(vmem, vmem, vmem, vmem),
        scratch_shapes=[
            pltpu.VMEM((64, 128, 256), BF16),
            pltpu.VMEM((256, 1024), BF16),
            pltpu.VMEM((2048, 768), BF16),
            pltpu.VMEM((768, 1024), BF16),
            pltpu.VMEM((512, 768), BF16),
            pltpu.VMEM((2, 16, 256), F32),
            pltpu.VMEM((2, 16, 256), BF16),
            pltpu.VMEM((2, 8, 16, 256), BF16),
            pltpu.VMEM((2, 16, 256), BF16),
            pltpu.VMEM((2, 16, 256), BF16),
            pltpu.VMEM((8, 8, 1024), F32),
            pltpu.VMEM((8, 8, 1024), BF16),
            pltpu.VMEM((8, 8, 1024), BF16),
            pltpu.VMEM((8, 1024), BF16),
            pltpu.VMEM((8, 1024), BF16),
            pltpu.VMEM((2, 4, 4, 4, 8, 1024), BF16),
            dma((7,)), dma((2, 8)), dma((2, 8)), dma((8,)), dma((8,)), dma((2,)), dma((2,)),
            dma((3, 15)), dma((3, 16)), dma((3, 3)), dma((3, 4)), dma((3, 4)), dma((3, 4)),
        ],
        compiler_params=pltpu.CompilerParams(
            collective_id=0, has_side_effects=True, vmem_limit_bytes=36 * 2**20
        ),
    )(
        in_hbm(teacher_states), in_hbm(teacher_proj), teacher_gain.reshape(1, 256), tlive,
        in_hbm(sx), in_hbm(student_proj), sgain, slive, pos.reshape(32, 1),
    )
    grad_embed, grad_states = pl.pallas_call(
        back_kernel,
        name="back",
        out_shape=(jax.ShapeDtypeStruct((32, 1024), F32), jax.ShapeDtypeStruct((2048, 768), BF16)),
        in_specs=[vmem] * 7,
        out_specs=(hbm, hbm),
        scratch_shapes=[pltpu.VMEM((2048, 768), BF16), dma((9,))],
        compiler_params=pltpu.CompilerParams(vmem_limit_bytes=36 * 2**20),
    )(ge, praw, gp, sl, student_proj, sgain, sx)
    return grad_embed, grad_states.reshape(32, 64, 768)


def solution(mesh):
    in_specs = (
        P("dp", None, "mp"), P("mp"), P("mp", None), P("dp", None),
        P(("dp", "mp"), None, None), P(), P(), P(("dp", "mp"), None), P(("dp", "mp")),
    )
    out_specs = (P(("dp", "mp"), None), P(("dp", "mp"), None, None))
    return jax.shard_map(shards, mesh=mesh, in_specs=in_specs, out_specs=out_specs, check_vma=False)
```

```python
import functools

import jax
import jax.numpy as jnp
from jax import lax
from jax.experimental import pallas as pl
from jax.experimental.pallas import tpu as pltpu
from jax.sharding import PartitionSpec as P

D = 4096
F32 = jnp.float32
BF16 = jnp.bfloat16
MESH = pl.DeviceIdType.MESH
NT = (((1,), (1,)), ((), ()))
PARTS = ((0, 384), (384, 384), (768, 256))
GELU_C = 0.7978845608028654
GELU_K = 0.044715


def place():
    d, m = lax.axis_index("dp"), lax.axis_index("mp")
    return d >> 2, d & 3, m >> 3, (m >> 1) & 3, m & 1


def student_chunk(i, sx, sproj, sgain, mask, gp, praw, sl_out, normed):
    rows = pl.ds(i * 512, 512)
    diagonal = lax.broadcasted_iota(jnp.int32, (64, 64), 0) == lax.broadcasted_iota(jnp.int32, (64, 64), 1)
    live = mask[8 * i : 8 * i + 8, :].astype(F32)
    live = jnp.where(diagonal[None], live[:, None, :], 0.0).reshape(512, 64)
    live = jnp.sum(live, axis=1, keepdims=True)
    x = sx[rows, :].astype(F32)
    scale = lax.rsqrt(jnp.sum(x * x, axis=1, keepdims=True) / 768.0 + 1e-06)
    sl = scale * live
    sl_out[rows, :] = jnp.broadcast_to(sl, (512, 128))
    normed[...] = (x * sl * sgain[...].reshape(1, 768)).astype(BF16)

    def block(n, carry):
        cols = pl.ds(pl.multiple_of(n * 256, 256), 256)
        pre = jnp.dot(normed[...], sproj[:, cols], preferred_element_type=F32)
        sq = pre * pre
        half = 0.5 + 0.5 * jnp.tanh(pre * (GELU_C + (GELU_C * GELU_K) * sq))
        act = pre * half
        gp[rows, cols] = (
            half + act * (1.0 - half) * (2.0 * GELU_C + (6.0 * GELU_C * GELU_K) * sq)
        ).astype(BF16)
        praw[i * 8 : i * 8 + 8, cols] = jnp.sum(act.reshape(8, 64, 256), axis=1)
        return carry

    lax.fori_loop(0, 4, block, 0)


def gather_kernel(
    tx_hbm, tproj_hbm, tgain_hbm, tmask_hbm, sx_hbm, sproj_hbm, sgain_hbm, smask_hbm, pos_hbm,
    ge, gp, praw, sl_out, sgain, sx, sproj,
    tx, tproj, normed, tgain, tmask, smask, pos,
    sq_own, sq_out, sq_in, sqz_out, sqz_in,
    pe_own, pe_out, pe_in, pez_out, pez_in, T,
    tx_sem, ld_sem, sq_s, sq_r, pe_s, pe_r, z_s, z_r, a1_s, a1_r, a2_s, a2_r, c_s, c_r,
):
    zlo, x, zhi, y, core = place()
    z = zhi * 4 + zlo
    two = 2 - 4 * core

    def dev(zz, xx, yy, cc):
        zz, xx, yy = (zz + 8) & 7, xx & 3, yy & 3
        return {"dp": (zz & 3) * 4 + xx, "mp": (zz >> 2) * 8 + yy * 2 + cc}

    loads = []
    for k in range(8):
        part = pl.ds(32 * (k // 4) + 16 * (k % 2) + 8 * (k // 2 % 2), 8)
        loads.append(pltpu.make_async_copy(tx_hbm.at[part], tx.at[part], tx_sem.at[k]))
    loads.append(pltpu.make_async_copy(sx_hbm, sx, ld_sem.at[4]))
    loads.append(pltpu.make_async_copy(sproj_hbm, sproj, ld_sem.at[5]))
    loads.append(pltpu.make_async_copy(tproj_hbm, tproj, ld_sem.at[6]))
    loads.append(pltpu.make_async_copy(sgain_hbm, sgain, ld_sem.at[7]))
    loads.append(pltpu.make_async_copy(smask_hbm, smask, ld_sem.at[8]))
    loads.append(pltpu.make_async_copy(tgain_hbm, tgain, ld_sem.at[9]))
    loads.append(pltpu.make_async_copy(tmask_hbm, tmask, ld_sem.at[10]))
    loads.append(pltpu.make_async_copy(pos_hbm, pos, ld_sem.at[11]))
    for c in loads[:8]:
        c.start()

    peers = [dev(z, x, y + dy, cc) for dy in range(4) for cc in (core, 1 - core)][1:]
    peers.append(dev(z + 4, x, y, core))
    for dz in (0, 1, -1, 2, -2):
        for dy in range(4):
            if dz:
                peers.append(dev(z + dz, x, y + dy, core))
        for dx in range(1, 4):
            peers.append(dev(z + dz, x + dx, y, core))
    for dx in range(1, 4):
        for dy in range(1, 4):
            peers.append(dev(z, x + dx, y + dy, core))
    barrier = pltpu.get_barrier_semaphore()
    for p in peers:
        pl.semaphore_signal(barrier, inc=1, device_id=p, device_id_type=MESH)

    def remote(src, dst, ss, rs, to):
        return pltpu.make_async_remote_copy(
            src_ref=src, dst_ref=dst, send_sem=ss, recv_sem=rs, device_id=to, device_id_type=MESH
        )

    me = y * 2 + core
    others = [(me + k) & 7 for k in range(1, 8)]
    sends = []

    def peer8(s):
        return dev(z, x, s >> 1, s & 1)

    def pair(h, q):
        p = 32 * h + q
        return jnp.concatenate([tx[p], tx[p + 16]], axis=0)

    row = lax.broadcasted_iota(jnp.int32, (16, 256), 0)
    for h in range(2):
        total = jnp.zeros((16, 256), F32)
        for q in range(16):
            if q % 8 == 0:
                loads[4 * h + 2 * (q // 8)].wait()
                loads[4 * h + 2 * (q // 8) + 1].wait()
                if h == 0 and q == 8:
                    for c in loads[8:]:
                        c.start()
            v = pair(h, q)
            pick = jnp.where(row == q, 1.0, 0.0).astype(BF16)
            total = total + lax.dot_general(pick, v * v, NT, preferred_element_type=F32)
        sq_own[h] = total
        sq_out[h] = total.astype(BF16)
        if h == 0:
            pl.semaphore_wait(barrier, len(peers))
        for s in others:
            c = remote(sq_out.at[h], sq_in.at[h, me], sq_s.at[h, s], sq_r.at[h, me], peer8(s))
            c.start()
            sends.append(c)

    for k in (8, 9, 11, 12):
        loads[k].wait()
    student = functools.partial(
        student_chunk, sx=sx, sproj=sproj, sgain=sgain, mask=smask, gp=gp, praw=praw, sl_out=sl_out, normed=normed
    )
    student(0)

    partner = dev(z + 4, x, y, core)
    for h in range(2):
        for s in others:
            remote(sq_in.at[h, s], sq_in.at[h, s], sq_s.at[h, s], sq_r.at[h, s], partner).wait_recv()
        total = sq_own[h]
        for s in others:
            total = total + sq_in[h, s].astype(F32)
        sq_own[h] = total
        sqz_out[h] = total.astype(BF16)
    zc = remote(sqz_out, sqz_in, z_s.at[0], z_r.at[0], partner)
    zc.start()
    sends.append(zc)
    student(1)
    zc.wait_recv()

    for k in (10, 13, 14, 15):
        loads[k].wait()
    row = lax.broadcasted_iota(jnp.int32, (32, 256), 0)
    lane = lax.broadcasted_iota(jnp.int32, (32, 256), 1)
    pooled = []
    for h in range(2):
        squares = sq_own[h] + sqz_in[h].astype(F32)
        live = jnp.concatenate([tmask[32 * h : 32 * h + 16, :], tmask[32 * h + 16 : 32 * h + 32, :]], axis=1)
        weight = live.astype(F32) * lax.rsqrt(squares / D + 1e-06)
        high = weight.astype(BF16).astype(F32)
        low = weight - high
        halves = []
        for g in range(2):
            total = jnp.zeros((32, 256), F32)
            for k in range(8):
                q = 8 * g + k
                both = jnp.where(row < 16, high[q : q + 1, :], low[q : q + 1, :])
                mine = (row & 15) == k + 8 * (lane >> 7)
                lhs = jnp.where(mine, both, 0.0).astype(BF16)
                total = total + jnp.dot(lhs, pair(h, q), preferred_element_type=F32)
            halves.append(total[:16] + total[16:])
        pooled += [halves[0][:8], halves[1][:8], halves[0][8:], halves[1][8:]]
    tpooled = (jnp.concatenate(pooled, axis=0) * tgain[...].reshape(1, 256)).astype(BF16)
    partial = jnp.dot(tpooled, tproj[...], preferred_element_type=F32).reshape(8, 8, 1024)
    pe_own[...] = partial
    pe_out[...] = partial.astype(BF16)
    for s in others:
        c = remote(pe_out.at[s], pe_in.at[me], pe_s.at[s], pe_r.at[me], peer8(s))
        c.start()
        sends.append(c)
    student(2)
    for s in others:
        remote(pe_in.at[s], pe_in.at[s], pe_s.at[s], pe_r.at[s], partner).wait_recv()
    total = pe_own[me]
    for s in others:
        total = total + pe_in[s].astype(F32)
    pez_out[...] = total.astype(BF16)
    zc = remote(pez_out, pez_in, z_s.at[1], z_r.at[1], partner)
    zc.start()
    sends.append(zc)
    student(3)
    zc.wait_recv()
    traw = total + pez_in[...].astype(F32)
    scale = lax.rsqrt(jnp.mean(traw * traw, axis=-1, keepdims=True) + 1e-06)
    T[core, zlo, x, y] = (traw * scale / 32.0).astype(BF16)

    zoffs = (0, 1, -1, two)
    ahead = lambda v, k: (v + k) & 3

    def plane(part, az, ax, ay):
        lo, n = PARTS[part]
        return T.at[core, az, ax, ay, :, pl.ds(lo, n)]

    slots = (zlo * 4 + y, zlo * 4 + x, x * 4 + y)
    for part in range(3):
        mine = plane(part, zlo, x, y)
        targets = []
        if part == 0:
            targets = [dev(z + zoffs[a], x, y + b, core) for a in range(4) for b in range(4) if a or b]
        elif part == 1:
            targets = [dev(z + zoffs[a], x + b, y, core) for a in range(4) for b in range(4) if a or b]
        else:
            targets = [dev(z, x + a, y + b, core) for a in range(4) for b in range(4) if a or b]
        for k, to in enumerate(targets):
            c = remote(mine, mine, a1_s.at[part, k], a1_r.at[part, slots[part]], to)
            c.start()
            sends.append(c)

    def line(part, cc, v):
        lo, n = PARTS[part]
        cols = pl.ds(lo, n)
        if part == 0:
            return T.at[cc, :, v, :, :, cols]
        if part == 1:
            return T.at[cc, :, :, v, :, cols]
        return T.at[cc, v, :, :, :, cols]

    own_line = (x, y, zlo)
    other = dev(z, x, y, 1 - core)
    for part in range(3):
        mine = plane(part, zlo, x, y)
        for k in range(1, 16):
            s = (slots[part] + k) & 15
            remote(mine, mine, a1_s.at[part, k - 1], a1_r.at[part, s], other).wait_recv()
        v = own_line[part]
        src = line(part, core, v)
        if part == 0:
            targets = [dev(z, x + k, y, core) for k in (1, 3, 2)]
        elif part == 1:
            targets = [dev(z, x, y + k, core) for k in (1, 3, 2)]
        else:
            targets = [dev(z + zoffs[k], x, y, core) for k in (1, 2, 3)]
        for k, to in enumerate(targets):
            c = remote(src, src, a2_s.at[part, k], a2_r.at[part, v], to)
            c.start()
            sends.append(c)
        c = remote(src, src, c_s.at[part, v], c_r.at[part, v], other)
        c.start()
        sends.append(c)
    for k in (1, 3, 2):
        for part in range(3):
            v = ahead(own_line[part], k)
            src = line(part, core, v)
            remote(src, src, a2_s.at[part, 0], a2_r.at[part, v], other).wait_recv()
            c = remote(src, src, c_s.at[part, v], c_r.at[part, v], other)
            c.start()
            sends.append(c)
    for part in range(3):
        for v in range(4):
            dst = line(part, 1 - core, v)
            remote(dst, dst, c_s.at[part, v], c_r.at[part, v], other).wait_recv()

    praws = praw[...]
    semb = praws * lax.rsqrt(jnp.mean(praws * praws, axis=-1, keepdims=True) + 1e-06) / 32.0
    temb = T[...].reshape(1024, 1024)
    lanes = lax.broadcasted_iota(jnp.int32, (32, 1024), 1)
    diagonal = lax.broadcasted_iota(jnp.int32, (32, 32), 0) == lax.broadcasted_iota(jnp.int32, (32, 32), 1)
    wanted = jnp.sum(jnp.where(diagonal, pos[...].reshape(1, 32), 0), axis=1, keepdims=True)
    wanted = ((wanted >> 3) & 1) * 512 + (wanted >> 8) * 128 + ((wanted >> 6) & 3) * 32 + ((wanted >> 4) & 3) * 8 + (wanted & 7)
    picker = jnp.where(wanted == lanes, 1.0, 0.0).astype(BF16)
    tpos = jnp.dot(picker, temb, preferred_element_type=F32).astype(BF16)
    both = jnp.concatenate([tpos, semb.astype(BF16)], axis=0)
    logits = lax.dot_general(both, temb, NT, preferred_element_type=F32)
    texp = jnp.exp(10.0 * logits[:32])
    sexp = jnp.exp(20.0 * logits[32:])
    diff = sexp / jnp.sum(sexp, axis=1, keepdims=True) - texp / jnp.sum(texp, axis=1, keepdims=True)
    ge[...] = 20.0 * jnp.dot(diff.astype(BF16), temb, preferred_element_type=F32)

    for c in sends:
        c.wait_send()


def back_kernel(ge, praw, gp, sl_in, sproj, sgain, sx, ge_hbm, out_hbm, out, st_sem):
    stores = [pltpu.make_async_copy(ge, ge_hbm, st_sem.at[8])]
    stores[0].start()
    p, g = praw[...], ge[...]
    r = lax.rsqrt(jnp.mean(p * p, axis=-1, keepdims=True) + 1e-06)
    ds = (g * r - p * (r * r * r) * jnp.mean(p * g, axis=-1, keepdims=True)) / 32.0
    gain = sgain[...].reshape(1, 768)
    for i in range(8):
        rows = pl.ds(256 * i, 256)
        slope = gp[rows, :].astype(F32).reshape(4, 64, 1024)
        dpre = (slope * ds[4 * i : 4 * i + 4][:, None, :]).reshape(256, 1024).astype(BF16)
        dn = lax.dot_general(dpre, sproj[...], NT, preferred_element_type=F32)
        dy = dn.astype(BF16).astype(F32) * gain
        x = sx[rows, :].astype(F32)
        sl = sl_in[rows, :1]
        m = jnp.sum(x * dy, axis=1, keepdims=True) * (sl * sl / 768.0)
        out[rows, :] = (sl * (dy - x * m)).astype(BF16)
        stores.append(pltpu.make_async_copy(out.at[rows], out_hbm.at[rows], st_sem.at[i]))
        stores[-1].start()
    for c in stores:
        c.wait()


def shards(
    teacher_states, teacher_gain, teacher_proj, teacher_mask,
    student_states, student_gain, student_proj, student_mask, positive,
):
    vmem = pl.BlockSpec(memory_space=pltpu.VMEM)
    hbm = pl.BlockSpec(memory_space=pltpu.HBM)
    dma = pltpu.SemaphoreType.DMA
    in_hbm = lambda a: pltpu.with_memory_space_constraint(a, pltpu.HBM)
    ge, gp, praw, sl, sgain, sx, sproj = pl.pallas_call(
        gather_kernel,
        name="gather",
        out_shape=(
            jax.ShapeDtypeStruct((32, 1024), F32),
            jax.ShapeDtypeStruct((2048, 1024), BF16),
            jax.ShapeDtypeStruct((32, 1024), F32),
            jax.ShapeDtypeStruct((2048, 128), F32),
            jax.ShapeDtypeStruct((768,), F32),
            jax.ShapeDtypeStruct((2048, 768), BF16),
            jax.ShapeDtypeStruct((768, 1024), BF16),
        ),
        in_specs=[hbm] * 9,
        out_specs=(vmem,) * 7,
        scratch_shapes=[
            pltpu.VMEM((64, 128, 256), BF16),
            pltpu.VMEM((256, 1024), BF16),
            pltpu.VMEM((512, 768), BF16),
            pltpu.VMEM((256,), F32),
            pltpu.VMEM((64, 128), jnp.int32),
            pltpu.VMEM((32, 64), jnp.int32),
            pltpu.VMEM((32,), jnp.int32),
            pltpu.VMEM((2, 16, 256), F32),
            pltpu.VMEM((2, 16, 256), BF16),
            pltpu.VMEM((2, 8, 16, 256), BF16),
            pltpu.VMEM((2, 16, 256), BF16),
            pltpu.VMEM((2, 16, 256), BF16),
            pltpu.VMEM((8, 8, 1024), F32),
            pltpu.VMEM((8, 8, 1024), BF16),
            pltpu.VMEM((8, 8, 1024), BF16),
            pltpu.VMEM((8, 1024), BF16),
            pltpu.VMEM((8, 1024), BF16),
            pltpu.VMEM((2, 4, 4, 4, 8, 1024), BF16),
            dma((8,)), dma((12,)), dma((2, 8)), dma((2, 8)), dma((8,)), dma((8,)), dma((2,)), dma((2,)),
            dma((3, 15)), dma((3, 16)), dma((3, 3)), dma((3, 4)), dma((3, 4)), dma((3, 4)),
        ],
        compiler_params=pltpu.CompilerParams(
            collective_id=0, has_side_effects=True, vmem_limit_bytes=36 * 2**20
        ),
    )(
        *map(in_hbm, (
            teacher_states, teacher_proj, teacher_gain, teacher_mask,
            student_states.reshape(2048, 768), student_proj, student_gain, student_mask, positive,
        )),
    )
    grad_embed, grad_states = pl.pallas_call(
        back_kernel,
        name="back",
        out_shape=(jax.ShapeDtypeStruct((32, 1024), F32), jax.ShapeDtypeStruct((2048, 768), BF16)),
        in_specs=[vmem] * 7,
        out_specs=(hbm, hbm),
        scratch_shapes=[pltpu.VMEM((2048, 768), BF16), dma((9,))],
        compiler_params=pltpu.CompilerParams(vmem_limit_bytes=36 * 2**20),
    )(ge, praw, gp, sl, sproj, sgain, sx)
    return grad_embed, grad_states.reshape(32, 64, 768)


def solution(mesh):
    in_specs = (
        P("dp", None, "mp"), P("mp"), P("mp", None), P("dp", None),
        P(("dp", "mp"), None, None), P(), P(), P(("dp", "mp"), None), P(("dp", "mp")),
    )
    out_specs = (P(("dp", "mp"), None), P(("dp", "mp"), None, None))
    return jax.shard_map(shards, mesh=mesh, in_specs=in_specs, out_specs=out_specs, check_vma=False)
```
